32 devices in a mesh: section: 2 (over core), seq: 4 (over y, x), head: 4 (over z).
Axes of the slice: x: 2, y: 2, z: 4, core: 2. Of those that a mesh axis runs over, the one named last changes fastest.
Arguments:
- x_in: bfloat16 [2, 1024, 8192], P('section', 'seq', 'head'), may hold values from -6 to 6
- b_in: bfloat16 [2, 1024, 2048], P('section', 'seq', 'head'), may hold values from -6 to 6
- c_in: bfloat16 [2, 1024, 2048], P('section', 'seq', 'head'), may hold values from -6 to 6
- z_in: bfloat16 [2, 1024, 8192], P('section', 'seq', 'head'), may hold values from -6 to 6
- dt_raw: float32 [2, 128, 1024], P('section', 'head', 'seq'), may hold values from -5 to 5
- conv_x: float32 [2, 4, 8192], P('section', None, 'head'), may hold values from -3 to 3
- conv_b: float32 [2, 4, 2048], P('section', None, 'head'), may hold values from -3 to 3
- conv_c: float32 [2, 4, 2048], P('section', None, 'head'), may hold values from -3 to 3
- a_rate: float32 [2, 128], P('section', 'head'), may hold values from 0.0001 to 1
- dt_bias: float32 [2, 128], P('section', 'head'), may hold values from -3 to -0.5
- skip_d: float32 [2, 128], P('section', 'head'), may hold values from 0.5 to 2
- norm_gain: float32 [2, 8192], P('section', 'head'), may hold values from 0.25 to 1.75
- out_weight: bfloat16 [2, 8192, 8192], P('section', 'head', 'seq'), may hold values from -0.0625 to 0.0625
Outputs:
- mixed: bfloat16 [2, 1024, 8192], P('section', ('seq', 'head'))
The draws below stay inside these ranges and needn't reach their ends.
All inputs are finite; a program needn't handle non-finite values.
Results may differ from the reference program's by a relative error of at most 0.007.
Values may be sent and summed in bfloat16 or wider, within the bound.
A program may use at most 128 MiB of HBM per device.

```python
import math
import jax
import jax.numpy as jnp
from jax import lax

D = 8192
P_SIZE = 64
N = 256
G = 8
KCONV = 4
HEADS = 128
TOK_DEV = 256
INNER = 8192
TOKENS = 1024
SECTIONS = 2


def draw_a_rate(key, part):
    lowest = math.log(0.0002)
    highest = math.log(1.0)
    exponent = jax.random.uniform(key, (SECTIONS, HEADS), jnp.float32, lowest, highest)
    return jnp.exp(exponent)


def level_of(key, shape, shards, low, top_value):
    level, own = 1.0, jax.random.fold_in(key, 6)
    for position, blocks in shards:
        draws = jnp.exp(jax.random.uniform(jax.random.fold_in(own, position), (blocks,), jnp.float32, low / len(shards), top_value / len(shards)))
        level = level * jnp.repeat(draws, shape[position] // blocks).reshape([-1 if axis == position else 1 for axis in range(len(shape))])
    return level


def gaussian(key, extent, width, bound, pieces=(), kind=jnp.bfloat16):
    gain = level_of(key, extent, pieces, -0.22, 0.18) if pieces else 1.0
    entries = jax.random.normal(key, extent, jnp.float32) * width * gain
    return jnp.minimum(jnp.maximum(entries, -bound), bound).astype(kind)


def setup_inputs(seed: int = 0) -> dict:
    key_of = jax.random.split(jax.random.key(seed), 14)
    return {
        "x_in": gaussian(key_of[0], (SECTIONS, TOKENS, INNER), 1.0, 6.0, ((0, 2), (1, 4), (2, 4))),
        "b_in": gaussian(key_of[1], (SECTIONS, TOKENS, G * N), 1.0, 6.0, ((0, 2), (1, 4), (2, 4))),
        "c_in": gaussian(key_of[2], (SECTIONS, TOKENS, G * N), 1.0, 6.0, ((0, 2), (1, 4), (2, 4))),
        "z_in": gaussian(key_of[3], (SECTIONS, TOKENS, INNER), 1.0, 6.0, ((0, 2), (1, 4), (2, 4))),
        "dt_raw": gaussian(key_of[4], (SECTIONS, HEADS, TOKENS), 1.0, 5.0, ((0, 2), (1, 4), (2, 4)), jnp.float32),
        "conv_x": gaussian(key_of[5], (SECTIONS, KCONV, INNER), KCONV ** -0.5, 3.0, ((0, 2), (2, 4)), jnp.float32),
        "conv_b": gaussian(key_of[6], (SECTIONS, KCONV, G * N), KCONV ** -0.5, 3.0, ((0, 2), (2, 4)), jnp.float32),
        "conv_c": gaussian(key_of[7], (SECTIONS, KCONV, G * N), KCONV ** -0.5, 3.0, ((0, 2), (2, 4)), jnp.float32),
        "a_rate": draw_a_rate(jax.random.fold_in(key_of[13], 71), 0),
        "dt_bias": jnp.clip(-3.0 + 2.5 * jax.random.uniform(key_of[9], (SECTIONS, HEADS), jnp.float32) ** level_of(key_of[9], (SECTIONS, HEADS), ((0, 2), (1, 4)), -0.2, 0.2), -3.0, -0.5),
        "skip_d": jnp.clip(0.5 + 1.5 * jax.random.uniform(key_of[10], (SECTIONS, HEADS), jnp.float32) ** level_of(key_of[10], (SECTIONS, HEADS), ((0, 2), (1, 4)), -0.2, 0.2), 0.5, 2.0),
        "norm_gain": jnp.clip(1.0 + 0.15 * jax.random.normal(key_of[11], (SECTIONS, INNER), jnp.float32), 0.25, 1.75),
        "out_weight": gaussian(key_of[12], (SECTIONS, INNER, D), INNER ** -0.5, 0.0625, ((0, 2), (1, 4), (2, 4))),
    }


epsilon = 1e-05

def conv_silu(signal, kernel):
    kernel_taps = kernel.shape[0]
    length = signal.shape[0]
    padded = jnp.pad(signal, ((kernel_taps - 1, 0), (0, 0)))
    summed = jnp.zeros(signal.shape, jnp.float32)
    for offset in range(kernel_taps):
        summed = summed + kernel[offset] * padded[offset:offset + length].astype(jnp.float32)
    return jax.nn.silu(summed).astype(jnp.bfloat16)

def one_layer(x_in, b_in, c_in, z_in, dt_raw, conv_x, conv_b, conv_c, a_rate, dt_bias, skip_d, norm_gain, out_weight):
    x_conv = conv_silu(x_in, conv_x)
    b_conv = conv_silu(b_in, conv_b)
    c_conv = conv_silu(c_in, conv_c)
    step_size = jax.nn.softplus(dt_raw + dt_bias[:, None])
    step_log = -a_rate[:, None] * step_size
    blocks = TOKENS // TOK_DEV
    per_group = HEADS // G
    x_blocks = x_conv.reshape(blocks, TOK_DEV, G, per_group, P_SIZE)
    b_blocks = b_conv.reshape(blocks, TOK_DEV, G, N)
    c_blocks = c_conv.reshape(blocks, TOK_DEV, G, N)
    z_blocks = z_in.reshape(blocks, TOK_DEV, INNER)
    step_blocks = jnp.transpose(step_size.reshape(G, per_group, blocks, TOK_DEV), (2, 0, 1, 3))
    log_blocks = jnp.transpose(step_log.reshape(G, per_group, blocks, TOK_DEV), (2, 0, 1, 3))
    causal = jnp.arange(TOK_DEV)[:, None] >= jnp.arange(TOK_DEV)[None, :]
    skip_term = skip_d.reshape(G, per_group)

    def block_step(carried, inputs):
        x_block, b_block, c_block, z_block, step_block, log_block = inputs
        log_decay = jnp.cumsum(log_block, axis=2)
        scores = jnp.einsum('tgn,ugn->gtu', c_block.astype(jnp.float32), b_block.astype(jnp.float32))
        spread_log = log_decay[:, :, :, None] - log_decay[:, :, None, :]
        damping = jnp.where(causal, jnp.exp(jnp.minimum(spread_log, 0.0)), 0.0)
        weights = (damping * step_block[:, :, None, :] * scores[:, None]).astype(jnp.bfloat16)
        weights = lax.optimization_barrier(weights).astype(jnp.float32)
        inside = jnp.einsum('gjtu,ugjp->tgjp', weights, x_block.astype(jnp.float32))
        to_end = jnp.exp(log_decay[:, :, -1:] - log_decay) * step_block
        x_weighted = (x_block.astype(jnp.float32) * jnp.transpose(to_end, (2, 0, 1))[..., None]).astype(jnp.bfloat16)
        x_weighted = lax.optimization_barrier(x_weighted).astype(jnp.float32)
        block_sum = jnp.einsum('ugjp,ugn->gjpn', x_weighted, b_block.astype(jnp.float32))
        block_decay = jnp.exp(log_decay[:, :, -1])
        carried_b = lax.optimization_barrier(carried.astype(jnp.bfloat16)).astype(jnp.float32)
        outside = jnp.einsum('tgn,gjpn->tgjp', c_block.astype(jnp.float32), carried_b)
        outside = outside * jnp.transpose(jnp.exp(log_decay), (2, 0, 1))[..., None]
        out_ssm = inside + outside + skip_term[None, :, :, None] * x_block.astype(jnp.float32)
        gated = out_ssm.reshape(TOK_DEV, G, per_group * P_SIZE) * jax.nn.silu(z_block.astype(jnp.float32)).reshape(TOK_DEV, G, per_group * P_SIZE)
        inverse_rms = lax.rsqrt(lax.optimization_barrier(jnp.mean(gated * gated, axis=2, keepdims=True)) + epsilon)
        hidden = ((gated * inverse_rms).reshape(TOK_DEV, INNER) * norm_gain).astype(jnp.bfloat16)
        new_carried = block_decay[:, :, None, None] * carried + block_sum
        return (new_carried, hidden)
    start = jnp.zeros((G, per_group, P_SIZE, N), jnp.float32)
    final_state, hidden = lax.scan(block_step, start, (x_blocks, b_blocks, c_blocks, z_blocks, step_blocks, log_blocks))
    hidden = hidden.reshape(TOKENS, INNER)
    return jnp.dot(hidden, out_weight, preferred_element_type=jnp.float32).astype(jnp.bfloat16)

def reference(x_in, b_in, c_in, z_in, dt_raw, conv_x, conv_b, conv_c, a_rate, dt_bias, skip_d, norm_gain, out_weight):
    layers = []
    for section_index in range(SECTIONS):
        layers.append(one_layer(x_in[section_index], b_in[section_index], c_in[section_index], z_in[section_index], dt_raw[section_index], conv_x[section_index], conv_b[section_index], conv_c[section_index], a_rate[section_index], dt_bias[section_index], skip_d[section_index], norm_gain[section_index], out_weight[section_index]))
    stacked = jnp.stack(layers)
    return jnp.roll(stacked, 1, axis=0)
```

```python
import jax
import jax.numpy as jnp
from jax import lax
from jax.sharding import PartitionSpec as P

N = 256


epsilon = 1e-05


def passed_along(block, axis, distance):
    devices = range(lax.axis_size(axis))
    route = [(i - distance, i) for i in devices if i - distance in devices]
    return lax.ppermute(block, axis, route)


def entering(decay, block, axis):
    size, place = (lax.axis_size(axis), lax.axis_index(axis))
    decays = lax.all_gather(decay, axis)
    blocks = lax.all_gather(block.astype(jnp.bfloat16), axis)
    carried = jnp.zeros_like(block)
    for k in range(size - 1):
        after = decays[k][:, :, None, None] * carried + blocks[k].astype(jnp.float32)
        carried = jnp.where(k < place, after, carried)
    return carried


def passed_along_2(block, axis, distance):
    devices = range(lax.axis_size(axis))
    route = [((i - distance) % len(devices), i) for i in devices]
    return lax.ppermute(block, axis, route)


def conv_silu(padded, kernel, length):
    kernel_taps = kernel.shape[0]
    summed = jnp.zeros((length, padded.shape[1]), jnp.float32)
    for offset in range(kernel_taps):
        summed = summed + kernel[offset] * padded[offset : offset + length].astype(jnp.float32)
    return jax.nn.silu(summed).astype(jnp.bfloat16)


def per_device(
    x_in,
    b_in,
    c_in,
    z_in,
    dt_raw,
    conv_x,
    conv_b,
    conv_c,
    a_rate,
    dt_bias,
    skip_d,
    norm_gain,
    out_weight,
):
    x_local = x_in[0]
    b_local = b_in[0]
    c_local = c_in[0]
    length = x_local.shape[0]
    kernel_taps = conv_x.shape[1]
    x_cols = x_local.shape[1]
    b_cols = b_local.shape[1]
    edge_rows = jnp.concatenate(
        [
            x_local[length - kernel_taps + 1 :],
            b_local[length - kernel_taps + 1 :],
            c_local[length - kernel_taps + 1 :],
        ],
        axis=1,
    )
    before = passed_along(edge_rows, "seq", 1)
    x_conv = conv_silu(jnp.concatenate([before[:, :x_cols], x_local], axis=0), conv_x[0], length)
    b_conv = conv_silu(
        jnp.concatenate([before[:, x_cols : x_cols + b_cols], b_local], axis=0), conv_b[0], length
    )
    c_conv = conv_silu(
        jnp.concatenate([before[:, x_cols + b_cols :], c_local], axis=0), conv_c[0], length
    )
    head_count = dt_raw.shape[1]
    group_count = b_cols // N
    per_group = head_count // group_count
    head_dim = x_cols // head_count
    step_size = jax.nn.softplus(dt_raw[0] + dt_bias[0][:, None])
    log_decay = jnp.cumsum(-a_rate[0][:, None] * step_size, axis=1)
    x_groups = x_conv.reshape(length, group_count, per_group, head_dim)
    b_groups = b_conv.reshape(length, group_count, N)
    c_groups = c_conv.reshape(length, group_count, N)
    log_groups = log_decay.reshape(group_count, per_group, length)
    step_groups = step_size.reshape(group_count, per_group, length)
    scores = jnp.einsum("tgn,ugn->gtu", c_groups, b_groups, preferred_element_type=jnp.float32)
    causal = jnp.arange(length)[:, None] >= jnp.arange(length)[None, :]
    spread_log = log_groups[:, :, :, None] - log_groups[:, :, None, :]
    damping = jnp.where(causal, jnp.exp(jnp.minimum(spread_log, 0.0)), 0.0)
    weights = (damping * step_groups[:, :, None, :] * scores[:, None]).astype(jnp.bfloat16)
    inside = jnp.einsum("gjtu,ugjp->tgjp", weights, x_groups, preferred_element_type=jnp.float32)
    to_end = jnp.exp(log_groups[:, :, -1:] - log_groups) * step_groups
    x_weighted = (
        x_groups.astype(jnp.float32) * jnp.transpose(to_end, (2, 0, 1))[..., None]
    ).astype(jnp.bfloat16)
    block_sum = jnp.einsum(
        "ugjp,ugn->gjpn", x_weighted, b_groups, preferred_element_type=jnp.float32
    )
    block_decay = jnp.exp(log_groups[:, :, -1])
    carried = entering(block_decay, block_sum, "seq")
    carried_b = carried.astype(jnp.bfloat16)
    outside = jnp.einsum("tgn,gjpn->tgjp", c_groups, carried_b, preferred_element_type=jnp.float32)
    outside = outside * jnp.transpose(jnp.exp(log_groups), (2, 0, 1))[..., None]
    skip_term = skip_d[0].reshape(group_count, per_group)
    out_ssm = inside + outside + skip_term[None, :, :, None] * x_groups.astype(jnp.float32)
    gate_act = jax.nn.silu(z_in[0].astype(jnp.float32)).reshape(
        length, group_count, per_group * head_dim
    )
    gated = out_ssm.reshape(length, group_count, per_group * head_dim) * gate_act
    inverse_rms = lax.rsqrt(jnp.mean(gated * gated, axis=2, keepdims=True) + epsilon)
    hidden = ((gated * inverse_rms).reshape(length, x_cols) * norm_gain[0]).astype(jnp.bfloat16)
    local_weight = out_weight[0]
    terms = jnp.dot(
        lax.all_gather(hidden, "seq", axis=0, tiled=True),
        local_weight,
        preferred_element_type=jnp.float32,
    )
    shards = lax.axis_size("seq")
    terms = terms.astype(jnp.bfloat16).reshape(shards, length, local_weight.shape[1])
    summed = lax.psum_scatter(terms, "head", scatter_dimension=1, tiled=True)
    spread = lax.all_to_all(summed, "seq", split_axis=0, concat_axis=2, tiled=True)
    mixed = spread.reshape(spread.shape[1], spread.shape[2])
    passed = passed_along_2(mixed, "section", 1)
    return passed[None]


def solution(mesh):
    return jax.shard_map(
        per_device,
        mesh=mesh,
        in_specs=(
            P("section", "seq", "head"),
            P("section", "seq", "head"),
            P("section", "seq", "head"),
            P("section", "seq", "head"),
            P("section", "head", "seq"),
            P("section", None, "head"),
            P("section", None, "head"),
            P("section", None, "head"),
            P("section", "head"),
            P("section", "head"),
            P("section", "head"),
            P("section", "head"),
            P("section", "head", "seq"),
        ),
        out_specs=P("section", ("seq", "head"), None),
        check_vma=False,
    )
```

```python
import functools

import jax
import jax.numpy as jnp
from jax import lax
from jax.experimental import pallas as pl
from jax.experimental.pallas import tpu as pltpu
from jax.sharding import PartitionSpec as P

N = 256


epsilon = 1e-05


def passed_along(block, axis, distance):
    devices = range(lax.axis_size(axis))
    route = [(i - distance, i) for i in devices if i - distance in devices]
    return lax.ppermute(block, axis, route)


def entering(decay, block, axis):
    size, place = (lax.axis_size(axis), lax.axis_index(axis))
    decays = lax.all_gather(decay, axis)
    blocks = lax.all_gather(block.astype(jnp.bfloat16), axis)
    carried = jnp.zeros_like(block)
    for k in range(size - 1):
        after = decays[k][:, :, None, None] * carried + blocks[k].astype(jnp.float32)
        carried = jnp.where(k < place, after, carried)
    return carried


def partner(place, bits):
    bit = 1
    while bit <= bits:
        if bits & bit:
            place = place + bit - 2 * bit * ((place // bit) % 2)
        bit *= 2
    return place


def project_kernel(
    sizes, hid, weight, out, w_buf, got, part, landed, summed,
    w_sem, ag_send, ag_recv, z_send, z_recv, o_send, o_recv,
):
    sections, shards, heads = sizes
    halves, count, _ = hid.shape
    rows, width = part.shape[3], part.shape[4]
    tile = min(512, width)
    here_s, here_h = lax.axis_index("seq"), lax.axis_index("head")
    other = lax.rem(lax.axis_index("section") + 1, sections)
    load = pltpu.make_async_copy(weight, w_buf, w_sem)
    load.start()
    barrier = pltpu.get_barrier_semaphore()
    for d in range(shards):
        if d:
            pl.semaphore_signal(barrier, inc=1, device_id={"seq": partner(here_s, d)})
        pl.semaphore_signal(
            barrier, inc=1, device_id={"section": other, "seq": partner(here_s, d)}
        )
    for e in range(1, heads):
        pl.semaphore_signal(barrier, inc=1, device_id={"head": partner(here_h, e)})
    pl.semaphore_wait(barrier, 2 * shards - 1 + heads - 1)

    def gather(q, d):
        return pltpu.make_async_remote_copy(
            hid.at[q], got.at[q, d - 1], ag_send.at[q, d], ag_recv.at[q, d],
            device_id={"seq": partner(here_s, d)},
        )

    def exchange(q, d, e):
        return pltpu.make_async_remote_copy(
            part.at[q, d, partner(here_h, e)], landed.at[q, d, e - 1],
            z_send.at[q, d, e], z_recv.at[q, d, e],
            device_id={"head": partner(here_h, e)},
        )

    def deliver(q, d):
        return pltpu.make_async_remote_copy(
            summed.at[q, d], out.at[q, here_s], o_send.at[q, d], o_recv.at[q, d],
            device_id={"section": other, "seq": partner(here_s, d)},
        )

    for q in range(halves):
        for d in range(1, shards):
            gather(q, d).start()
    load.wait()

    def multiply(q, d):
        rows_in = hid.at[q] if d == 0 else got.at[q, d - 1]

        def one(i, _):
            cols = pl.ds(pl.multiple_of(i * tile, tile), tile)
            terms = jnp.dot(rows_in[...], w_buf[:, cols], preferred_element_type=jnp.float32)
            part[q, d, :, :, cols] = terms.astype(jnp.bfloat16).reshape(heads, rows, tile)
            return 0

        lax.fori_loop(0, width // tile, one, 0)

    def finish(q, d):
        total = part[q, d, here_h].astype(jnp.float32)
        for e in range(1, heads):
            exchange(q, d, e).wait_recv()
            total = total + landed[q, d, e - 1].astype(jnp.float32)
        summed[q, d] = total.astype(jnp.bfloat16)
        deliver(q, d).start()

    units = [(q, 0) for q in range(halves)]
    units += [(q, d) for q in range(halves) for d in range(1, shards)]
    lag = 2
    for n, (q, d) in enumerate(units):
        if d:
            gather(q, d).wait_recv()
        multiply(q, d)
        for e in range(1, heads):
            exchange(q, d, e).start()
        if n >= lag:
            finish(*units[n - lag])
    for unit in units[len(units) - lag :]:
        finish(*unit)
    for q, d in units:
        if d:
            gather(q, d).wait_send()
        for e in range(1, heads):
            exchange(q, d, e).wait_send()
        deliver(q, d).wait_send()
        pltpu.make_async_remote_copy(
            summed.at[q, d], out.at[q, partner(here_s, d)], o_send.at[q, d], o_recv.at[q, d],
            device_id={"section": other, "seq": partner(here_s, d)},
        ).wait_recv()


def project(hid, weight, sizes):
    sections, shards, heads = sizes
    halves, count, depth = hid.shape
    width = weight.shape[1]
    rows = count // heads
    bf16 = jnp.bfloat16
    dma = pltpu.SemaphoreType.DMA
    flops = 2 * halves * count * shards * depth * width
    return pl.pallas_call(
        functools.partial(project_kernel, sizes),
        out_shape=jax.ShapeDtypeStruct((halves, shards, rows, width), bf16),
        in_specs=[pl.BlockSpec(memory_space=pltpu.VMEM), pl.BlockSpec(memory_space=pl.ANY)],
        out_specs=pl.BlockSpec(memory_space=pl.ANY),
        scratch_shapes=[
            pltpu.VMEM(weight.shape, bf16),
            pltpu.VMEM((halves, shards - 1, count, depth), bf16),
            pltpu.VMEM((halves, shards, heads, rows, width), bf16),
            pltpu.VMEM((halves, shards, heads - 1, rows, width), bf16),
            pltpu.VMEM((halves, shards, rows, width), bf16),
            dma,
            dma((halves, shards)),
            dma((halves, shards)),
            dma((halves, shards, heads)),
            dma((halves, shards, heads)),
            dma((halves, shards)),
            dma((halves, shards)),
        ],
        compiler_params=pltpu.CompilerParams(
            collective_id=0, has_side_effects=True, vmem_limit_bytes=48 * 2**20
        ),
        cost_estimate=pl.CostEstimate(
            flops=flops, bytes_accessed=2 * weight.size, transcendentals=0
        ),
        name="project",
    )(hid, weight)


def conv_silu(padded, kernel, length):
    kernel_taps = kernel.shape[0]
    summed = jnp.zeros((length, padded.shape[1]), jnp.float32)
    for offset in range(kernel_taps):
        summed = summed + kernel[offset] * padded[offset : offset + length].astype(jnp.float32)
    return jax.nn.silu(summed).astype(jnp.bfloat16)


def per_device(
    x_in,
    b_in,
    c_in,
    z_in,
    dt_raw,
    conv_x,
    conv_b,
    conv_c,
    a_rate,
    dt_bias,
    skip_d,
    norm_gain,
    out_weight,
):
    x_local = x_in[0]
    b_local = b_in[0]
    c_local = c_in[0]
    length = x_local.shape[0]
    kernel_taps = conv_x.shape[1]
    x_cols = x_local.shape[1]
    b_cols = b_local.shape[1]
    edge_rows = jnp.concatenate(
        [
            x_local[length - kernel_taps + 1 :],
            b_local[length - kernel_taps + 1 :],
            c_local[length - kernel_taps + 1 :],
        ],
        axis=1,
    )
    before = passed_along(edge_rows, "seq", 1)
    x_conv = conv_silu(jnp.concatenate([before[:, :x_cols], x_local], axis=0), conv_x[0], length)
    b_conv = conv_silu(
        jnp.concatenate([before[:, x_cols : x_cols + b_cols], b_local], axis=0), conv_b[0], length
    )
    c_conv = conv_silu(
        jnp.concatenate([before[:, x_cols + b_cols :], c_local], axis=0), conv_c[0], length
    )
    head_count = dt_raw.shape[1]
    group_count = b_cols // N
    per_group = head_count // group_count
    head_dim = x_cols // head_count
    step_size = jax.nn.softplus(dt_raw[0] + dt_bias[0][:, None])
    log_decay = jnp.cumsum(-a_rate[0][:, None] * step_size, axis=1)
    x_groups = x_conv.reshape(length, group_count, per_group, head_dim)
    b_groups = b_conv.reshape(length, group_count, N)
    c_groups = c_conv.reshape(length, group_count, N)
    log_groups = log_decay.reshape(group_count, per_group, length)
    step_groups = step_size.reshape(group_count, per_group, length)
    scores = jnp.einsum("tgn,ugn->gtu", c_groups, b_groups, preferred_element_type=jnp.float32)
    causal = jnp.arange(length)[:, None] >= jnp.arange(length)[None, :]
    spread_log = log_groups[:, :, :, None] - log_groups[:, :, None, :]
    damping = jnp.where(causal, jnp.exp(jnp.minimum(spread_log, 0.0)), 0.0)
    weights = (damping * step_groups[:, :, None, :] * scores[:, None]).astype(jnp.bfloat16)
    inside = jnp.einsum("gjtu,ugjp->tgjp", weights, x_groups, preferred_element_type=jnp.float32)
    to_end = jnp.exp(log_groups[:, :, -1:] - log_groups) * step_groups
    x_weighted = (
        x_groups.astype(jnp.float32) * jnp.transpose(to_end, (2, 0, 1))[..., None]
    ).astype(jnp.bfloat16)
    block_sum = jnp.einsum(
        "ugjp,ugn->gjpn", x_weighted, b_groups, preferred_element_type=jnp.float32
    )
    block_decay = jnp.exp(log_groups[:, :, -1])
    carried = entering(block_decay, block_sum, "seq")
    carried_b = carried.astype(jnp.bfloat16)
    outside = jnp.einsum("tgn,gjpn->tgjp", c_groups, carried_b, preferred_element_type=jnp.float32)
    outside = outside * jnp.transpose(jnp.exp(log_groups), (2, 0, 1))[..., None]
    skip_term = skip_d[0].reshape(group_count, per_group)
    out_ssm = inside + outside + skip_term[None, :, :, None] * x_groups.astype(jnp.float32)
    gate_act = jax.nn.silu(z_in[0].astype(jnp.float32)).reshape(
        length, group_count, per_group * head_dim
    )
    gated = out_ssm.reshape(length, group_count, per_group * head_dim) * gate_act
    inverse_rms = lax.rsqrt(jnp.mean(gated * gated, axis=2, keepdims=True) + epsilon)
    hidden = ((gated * inverse_rms).reshape(length, x_cols) * norm_gain[0]).astype(jnp.bfloat16)
    sizes = tuple(lax.axis_size(name) for name in ("section", "seq", "head"))
    halves, heads = 2, sizes[2]
    rows = length // (heads * halves)
    hid = jnp.transpose(hidden.reshape(heads, halves, rows, x_cols), (1, 0, 2, 3))
    mixed = project(hid.reshape(halves, heads * rows, x_cols), out_weight[0], sizes)
    return jnp.transpose(mixed, (0, 2, 1, 3)).reshape(1, halves * rows, -1)


def solution(mesh):
    return jax.shard_map(
        per_device,
        mesh=mesh,
        in_specs=(
            P("section", "seq", "head"),
            P("section", "seq", "head"),
            P("section", "seq", "head"),
            P("section", "seq", "head"),
            P("section", "head", "seq"),
            P("section", None, "head"),
            P("section", None, "head"),
            P("section", None, "head"),
            P("section", "head"),
            P("section", "head"),
            P("section", "head"),
            P("section", "head"),
            P("section", "head", "seq"),
        ),
        out_specs=P("section", ("seq", "head"), None),
        check_vma=False,
    )
```
